32 devices in a mesh: gx: 4 (over y, core), gy: 4 (over z), gz: 2 (over x).
Axes of the slice: x: 2, y: 2, z: 4, core: 2. Of those that a mesh axis runs over, the one named last changes fastest.
Arguments:
- spin_vectors: float32 [2, 3, 32, 32, 256], P(None, None, 'gx', 'gy', 'gz'), may hold values from -1 to 1, as said below
- displacement: float32 [2, 3, 32, 32, 256], P(None, None, 'gx', 'gy', 'gz'), may hold values from -0.15 to 0.15
- occupied: int32 [2, 32, 32, 256], P(None, 'gx', 'gy', 'gz'), may hold values 0 or 1
- applied_field: float32 [3], replicated, may hold values from -4 to 4
Outputs:
- new_spins: float32 [2, 3, 32, 32, 256], P(None, None, 'gx', 'gy', 'gz')
- forces: float32 [2, 3, 32, 32, 256], P(None, None, 'gx', 'gy', 'gz')
The draws below stay inside these ranges and needn't reach their ends.
Inputs may be any that keep to these rules, and one draw needn't show every extreme that they name: `occupied`: 1 where a lattice site holds an atom, 0 at a vacancy. `spin_vectors`: every spin vector has unit length.
All inputs are finite; a program needn't handle non-finite values. No bound on the sum of `occupied` on one device may be relied on, other than what follows from the above.
Results may differ from the reference program's by a relative error of at most 0.0001.
Values sent between devices are 32-bit elements; how exact they have to be, the bound alone decides.
A program may use at most 64 MiB of HBM per device.

```python
import math
import jax
import jax.numpy as jnp
from jax import lax

CX = 8
CY = 8
NX = 32
NY = 32
NZ = 256


def draw_spin_vectors(key, part):
    height_key, azimuth_key = jax.random.split(jax.random.fold_in(key, 11))
    extent = (2, NX, NY, NZ)
    height = jax.random.uniform(height_key, extent, jnp.float32, -1.0, 1.0)
    azimuth = jax.random.uniform(azimuth_key, extent, jnp.float32, -math.pi, math.pi)
    radius = jnp.sqrt(jnp.maximum(1.0 - height * height, 0.0))
    return jnp.stack([radius * jnp.cos(azimuth), radius * jnp.sin(azimuth), height], axis=1)


def with_ends(values, rng, low, largest):
    shape = values.shape
    index_at = [jax.random.randint(jax.random.fold_in(rng, axis), (), 0, shape[axis]) for axis in range(len(shape))]
    values = values.at[tuple(index_at)].set(low)
    longest = shape.index(max(shape))
    index_at[longest] = (index_at[longest] + 1) % shape[longest]
    return values.at[tuple(index_at)].set(largest)


def block_scale(key, dims, cuts, smallest, top_value):
    def one(axis_at, blocks):
        heights = jax.random.uniform(jax.random.fold_in(jax.random.fold_in(key, 6), axis_at), (blocks,), jnp.float32, smallest / len(cuts), top_value / len(cuts))
        return jnp.repeat(jnp.exp(heights), dims[axis_at] // blocks).reshape((-1,) + (1,) * (len(dims) - axis_at - 1))

    level = one(*cuts[0])
    for cut in cuts[1:]:
        level = level * one(*cut)
    return level


def centred(key, shape, width, limit, shards=(), kind=jnp.bfloat16):
    entries = jax.random.normal(key, shape, jnp.float32) * width
    if len(shards) > 0:
        entries = block_scale(key, shape, shards, -0.22, 0.18) * entries
    return jnp.clip(entries, min=-limit, max=limit).astype(kind)


def setup_inputs(seed: int = 0) -> dict:
    key_list = jax.random.split(jax.random.key(seed), 5)
    spin_vectors = draw_spin_vectors(jax.random.fold_in(key_list[4], 71), 0)
    displacement = centred(key_list[1], (2, 3, NX, NY, NZ), 0.04, 0.15, ((2, 4), (3, 4), (4, 2)), jnp.float32)
    occupied = with_ends((jax.random.randint(key_list[2], (2, NX, NY, NZ), 0, 16) < 15).astype(jnp.int32), jax.random.fold_in(key_list[2], 1), 0, 1)
    applied_field = centred(key_list[3], (3,), 1.0, 4.0, (), jnp.float32)
    return {"spin_vectors": spin_vectors, "displacement": displacement, "occupied": occupied, "applied_field": applied_field}


step_time = 0.6
exchange_scale = 0.35
exchange_decay = 4.0
pair_scale = 0.5
pair_decay = 6.0
density_decay = 3.0
bond_length = 0.8660254037844386
corner_offsets = [(a, b, c) for a in (0, 1) for b in (0, 1) for c in (0, 1)]

def roll_cells(values, offset, sign):
    return jnp.roll(values, tuple((sign * o for o in offset)), axis=(-3, -2, -1))

def cross_product(left, right):
    return jnp.stack([left[1] * right[2] - left[2] * right[1], left[2] * right[0] - left[0] * right[2], left[0] * right[1] - left[1] * right[0]])

def rotate(spin_state, torque, fraction):
    rotation = 0.5 * fraction * torque
    first_turn = cross_product(rotation, spin_state)
    second_turn = cross_product(rotation, first_turn)
    factor = 2.0 / (1.0 + lax.optimization_barrier(jnp.sum(rotation * rotation, axis=0)))
    return spin_state + factor * (first_turn + second_turn)

def geometry(displacement, occupancy, offset):
    partner = roll_cells(displacement[1], offset, 1)
    vector = jnp.stack([0.5 - offset[i] + partner[i] - displacement[0][i] for i in range(3)])
    length = jnp.sqrt(lax.optimization_barrier(jnp.sum(vector * vector, axis=0)))
    weight = occupancy[0] * roll_cells(occupancy[1], offset, 1)
    return (vector, length, weight)

def reference(spin_vectors, displacement, occupied, applied_field):
    occupancy = occupied.astype(jnp.float32)
    external = applied_field[:, None, None, None]
    cell_x = jnp.arange(spin_vectors.shape[2])[:, None, None]
    cell_y = jnp.arange(spin_vectors.shape[3])[None, :, None]
    x_half = cell_x // (CX // 2) % 2
    y_half = cell_y // (CY // 2) % 2
    couplings = []
    for offset in corner_offsets:
        vector, length, weight = geometry(displacement, occupancy, offset)
        couplings.append(weight * exchange_scale * jnp.exp(-exchange_decay * (length - bond_length)))
    current = spin_vectors
    for update in range(15):
        sector = update if update < 8 else 14 - update
        sublattice = sector % 2
        quarter = sector // 2
        fraction = step_time if update == 7 else 0.5 * step_time
        torque = external
        for corner, offset in enumerate(corner_offsets):
            if sublattice == 0:
                torque = torque + couplings[corner][None] * roll_cells(current[1], offset, 1)
            else:
                torque = torque + roll_cells(couplings[corner][None] * current[0], offset, -1)
        chosen = current[sublattice]
        turned = rotate(chosen, torque, fraction)
        inside = (x_half == quarter % 2) & (y_half == quarter // 2)
        turned = jnp.where(inside[None], turned, chosen)
        current = current.at[sublattice].set(turned)
    first_density = jnp.zeros(spin_vectors.shape[2:], jnp.float32)
    second_density = jnp.zeros(spin_vectors.shape[2:], jnp.float32)
    for offset in corner_offsets:
        vector, length, weight = geometry(displacement, occupancy, offset)
        density = weight * jnp.exp(-density_decay * (length - bond_length))
        first_density = first_density + density
        second_density = second_density + roll_cells(density, offset, -1)
    first_slope = -0.5 / jnp.sqrt(1.0 + first_density)
    second_slope = -0.5 / jnp.sqrt(1.0 + second_density)
    first_force = jnp.zeros(spin_vectors.shape[1:], jnp.float32)
    second_force = jnp.zeros(spin_vectors.shape[1:], jnp.float32)
    for corner, offset in enumerate(corner_offsets):
        vector, length, weight = geometry(displacement, occupancy, offset)
        stretch = length - bond_length
        alignment = lax.optimization_barrier(jnp.sum(current[0] * roll_cells(current[1], offset, 1), axis=0))
        slopes = first_slope + roll_cells(second_slope, offset, 1)
        strength = -pair_decay * pair_scale * weight * jnp.exp(-pair_decay * stretch) - density_decay * weight * jnp.exp(-density_decay * stretch) * slopes + exchange_decay * couplings[corner] * alignment
        bond_force = strength[None] * vector / length[None]
        first_force = first_force + bond_force
        second_force = second_force - roll_cells(bond_force, offset, -1)
    return (current, jnp.stack([first_force, second_force]))
```

```python
import functools
import itertools

import jax
import jax.numpy as jnp
from jax import lax
from jax.experimental import pallas as pl
from jax.experimental.pallas import tpu as pltpu
from jax.sharding import PartitionSpec as P

step_time = 0.6
exchange_scale = 0.35
exchange_decay = 4.0
pair_scale = 0.5
pair_decay = 6.0
density_decay = 3.0
bond_length = 0.8660254037844386
corner_offsets = list(itertools.product((0, 1), repeat=3))
axes = ("gx", "gy", "gz")
MESH = pl.DeviceIdType.MESH

DISPLACED, SPUN = 0, 1
GROUPS = ((0, 4), (9, 3))
ARRAYS = 16
S0, D0, S1, D1, FS = 0, 3, 6, 9, 12
PLACE = {w: w - w // 7 for w in range(14) if w % 7 != 6}
SENSE = (-1,) * 3 + (0,) * 3 + (1,) * 7
FAR = 1000.0


def fields_of(group):
    first, n = GROUPS[group]
    return [(first + n * s + f, 7 * s + f + (3 if group == DISPLACED else 0), s) for s in range(2) for f in range(n)]


def strip_of(group):
    first, n = GROUPS[group]
    return first + 2 * n


TO_BELOW = tuple(
    [(i // 4, i, 0, 2, 2 * (i % 4)) for i in range(8)] + [(2, 2 + i, 2, 2, 2 * i) for i in range(4)])
TO_ABOVE_0 = tuple([(0, i, 7, 1, i) for i in range(8)] + [(1, 2 + i, 5, 2, 2 * i) for i in range(4)])
TO_ABOVE_1 = tuple(
    [(i // 4, i, 6, 2, 2 * (i % 4)) for i in range(8)] + [(2, 2 + i, 4, 2, 2 * i) for i in range(4)])


@functools.cache
def turned_planes():
    need = {(0, x, y) for x in range(9) for y in range(9)} | {(1, x, y) for x in range(-1, 8) for y in range(-1, 8)}
    need |= {(b, x, y) for b in (0, 1) for x in range(8) for y in range(8)}
    planes = {}
    for u in reversed(range(15)):
        sector = u if u < 8 else 14 - u
        sub, quarter = sector % 2, sector // 2
        turned = [k for k in need if k[0] == sub and k[1] // 4 % 2 + 2 * (k[2] // 4 % 2) == quarter]
        planes[u] = sorted({k[1] for k in turned})
        for _, x, y in turned:
            for a, b, _ in corner_offsets:
                need.add((1, x - a, y - b) if sub == 0 else (0, x + a, y + b))
    return planes


def working():
    rows = 8
    row = lax.broadcasted_iota(jnp.int32, (rows, 128), 0)
    first, last = row % 4 == 0, row % 4 == 3

    def turn(v, n):
        return pltpu.roll(v, n % rows, 0)

    def below(pair, tile):
        a, b = pair
        if tile == 0:
            return jnp.where(first, turn(b, 5), turn(a, 1))
        return jnp.where(first, turn(a, 1), turn(b, 1))

    def above(pair, tile):
        a, b = pair
        if tile == 0:
            return jnp.where(last, turn(b, -1), turn(a, -1))
        return jnp.where(last, turn(a, 3), turn(b, -1))

    return below, above


def place_rows():
    up, down, at, n_up, n_down = [], [], [], 0, 0
    for group in (DISPLACED, SPUN):
        for s in [s for _, _, s in fields_of(group)] + [1]:
            up.append(n_up)
            down.append(n_down)
            at.append(s)
            n_up += 2 + s
            n_down += 3
    return up + [n_up], down + [n_down], at


UP, DOWN, GEOMETRY = place_rows()


def kernel(sizes, spin_in, disp_in, occ_in, field_in, out_s, out_f, E, PZ, RZ, SU, RU, SD, RD, SX, RX, SC, RC, U, UZ, XR, XZ, N, NZ, NR, NX, HALO, LR, TMP, J, J1, P3, RI,
           F0, HP, ACC, spin, disp, occ, field, send_sem, recv_sem, load_sem):
    nx, ny, nz = sizes
    me = {a: lax.axis_index(a) for a in axes}
    count = dict(zip(axes, sizes))

    def peer(axis, step):
        n = count[axis]
        return {axis: lax.rem(me[axis] + (n + step), n)}

    peers = []
    for axis in axes:
        peers.append(peer(axis, 1))
        if count[axis] > 2:
            peers.append(peer(axis, -1))
    barrier = pltpu.get_barrier_semaphore()
    for p in peers:
        pl.semaphore_signal(barrier, inc=1, device_id=p, device_id_type=MESH)

    loads = [pltpu.make_async_copy(a, b, load_sem.at[i])
             for i, (a, b) in enumerate(((spin_in, spin), (disp_in, disp), (occ_in, occ)))]
    for c in loads:
        c.start()
    field_load = pltpu.make_async_copy(field_in, field, load_sem.at[3])
    field_load.start()
    for c in loads:
        c.wait()

    lane = lax.broadcasted_iota(jnp.int32, (8, 128), 1)
    row = lax.broadcasted_iota(jnp.int32, (8, 128), 0)
    upper = row < 4

    def swap(v):
        return pltpu.roll(v, 4, 0)

    def load_own(x, _):
        for group in (DISPLACED, SPUN):
            packed = jnp.zeros((8, 128), jnp.float32)
            for n, (e, w, s) in enumerate(fields_of(group)):
                f = w % 7
                if f < 3:
                    v = spin[s, f, x]
                elif f < 6:
                    v = disp[s, f - 3, x]
                else:
                    v = occ[s, x].astype(jnp.float32)
                E[e, x, 0] = v
                packed = jnp.where(lane // 16 == n, pltpu.roll(v, (8 + 16 * n) % 128, 1), packed)
            PZ[group, x] = packed
        return 0

    lax.fori_loop(0, 8, load_own, 0, unroll=2)
    inner = (row >= 2) & (row < 6)

    def routes(e):
        return ((SU, RU, UP[e], (TO_ABOVE_0, TO_ABOVE_1)[GEOMETRY[e]]), (SD, RD, DOWN[e], TO_BELOW))

    def pack_rows(e):
        own = [E[e, x, 0] for x in range(8)]
        for out, _unused, first, pieces in routes(e):
            tiles = {}
            for tile, x, low, n, to in pieces:
                v = pltpu.roll(own[x], (to - low) % 8, 0)
                tiles[tile] = jnp.where(row < to, tiles[tile], v) if to else v
            for tile, v in tiles.items():
                out[first + tile] = v
        SX[0, e] = jnp.where(inner, own[2], swap(own[3]))
        SX[1, e] = jnp.where(inner, own[4], swap(own[5]))

    def unpack_rows(e):
        rows = [jnp.zeros((8, 128), jnp.float32)] * 8
        for _unused, arrived, first, pieces in routes(e):
            for tile, x, low, n, to in pieces:
                v = pltpu.roll(arrived[first + tile], (low - to) % 8, 0)
                rows[x] = jnp.where((row >= low) & (row < low + n), v, rows[x])
        for x in range(8):
            E[e, x, 1] = swap(rows[x])
        SC[0, e] = jnp.where(inner, swap(rows[1]), rows[0])
        SC[1, e] = jnp.where(inner, swap(rows[7]), rows[6])

    def arrays_of(group):
        return range(GROUPS[group][0], strip_of(group) + 1)

    for group in (DISPLACED, SPUN):
        for e, _, _ in fields_of(group):
            pack_rows(e)
    pl.semaphore_wait(barrier, len(peers))

    def send(i, src, dst, to):
        c = pltpu.make_async_remote_copy(
            src_ref=src, dst_ref=dst, send_sem=send_sem.at[i], recv_sem=recv_sem.at[i],
            device_id=to, device_id_type=MESH)
        c.start()
        return c

    def exchange_y(i, lo, hi):
        up = pl.ds(UP[lo], UP[hi] - UP[lo])
        down = pl.ds(DOWN[lo], DOWN[hi] - DOWN[lo])
        return [
            send(i, SD.at[down], RD.at[down], peer("gy", -1)),
            send(i + 1, SU.at[up], RU.at[up], peer("gy", 1)),
        ]

    def exchange_x(i, lo, hi):
        part = pl.ds(lo, hi - lo)

        def plane(x):
            return E.at[part, pl.ds(x, 2), 0]

        return [
            send(i, plane(0), plane(8), peer("gx", -1)),
            send(i + 1, plane(6), plane(14), peer("gx", 1)),
            send(i + 2, SX.at[0, part], RX.at[0, part], peer("gx", -1)),
            send(i + 3, SX.at[1, part], RX.at[1, part], peer("gx", 1)),
        ]

    def exchange_z(i, group):
        found = [send(i, PZ.at[group], RZ.at[0, group], peer("gz", -1))]
        if nz > 2:
            found.append(send(i + 1, PZ.at[group], RZ.at[1, group], peer("gz", 1)))
        return found

    def take_strips(group, copies):
        for c in copies:
            c.wait()
        for x in range(8):
            v = RZ[0, group, x]
            if nz > 2:
                v = jnp.where(lane % 16 < 8, RZ[1, group, x], v)
            E[strip_of(group), x, 0] = v
        pack_rows(strip_of(group))

    def corner_copies(i, group):
        part = pl.ds(GROUPS[group][0], len(arrays_of(group)))
        return [send(i + n, SC.at[n, part], RC.at[n, part], peer("gx", 2 * n - 1)) for n in range(2)]

    z0 = exchange_z(0, DISPLACED)
    ys0 = exchange_y(4, GROUPS[0][0], strip_of(0))
    xs0 = exchange_x(12, GROUPS[0][0], strip_of(0))
    z1 = exchange_z(2, SPUN)
    ys1 = exchange_y(8, GROUPS[1][0], GROUPS[1][0] + 1)
    xs1 = exchange_x(20, GROUPS[1][0], strip_of(1))
    take_strips(DISPLACED, z0)
    ys0 += exchange_y(6, strip_of(0), strip_of(0) + 1)
    ys1 += exchange_y(32, GROUPS[1][0] + 1, strip_of(1))
    xs0 += exchange_x(16, strip_of(0), strip_of(0) + 1)
    take_strips(SPUN, z1)
    ys1 += exchange_y(10, strip_of(1), strip_of(1) + 1)
    xs1 += exchange_x(24, strip_of(1), strip_of(1) + 1)

    below, above = working()
    segment = lane // 32
    third, quarter_low = lane % 16 >= 8, lane // 16

    def lane_roll(v, n):
        return pltpu.roll(v, n % 128, 1)

    def edge_of(halo, p, s):
        return lane_roll(halo, -(32 * p + 7) if s > 0 else 103 - 32 * p)

    def shifted(main, halo, p, s):
        return jnp.where(lane == (0 if s > 0 else 127), edge_of(halo, p, s), lane_roll(main, s))

    def spread(f, q, t, halo, s):
        U[f, 16 + q, t] = halo
        UZ[f, 16 + q, t] = lane_roll(halo, s)
        XR[f, q, t] = lane_roll(halo, 32 * s)
        XZ[f, q, t] = lane_roll(halo, 33 * s)

    def neighbour(now, other, s):
        return jnp.where(segment == (0 if s > 0 else 3), other, now)

    def halves(group, planes, j):
        fields = [(n, e, w) for n, (e, w, s) in enumerate(fields_of(group)) if w % 7 != 6]
        members = list(enumerate(fields_of(group)))
        groups = {}
        for x in planes:
            groups.setdefault(x // 4, []).append(x)
        lone = range(10, 14)

        def put(ref, kept, f, unit, v):
            if j == 0 and unit in lone:
                ref[f, unit, 0], ref[f, unit, 1] = v, v
            elif j == 0:
                kept[f, unit] = v
            else:
                own = kept[f, unit]
                ref[f, unit, 0], ref[f, unit, 1] = jnp.where(upper, own, v), jnp.where(upper, v, own)

        def main_of(x, e, w):
            if w % 7 == 3:
                return jnp.where(E[e + 3, x, j] > 0.5, E[e, x, j], FAR if w < 7 else -FAR)
            return E[e, x, j]

        for x in planes:
            for n, (e, w, _s) in members:
                TMP[n, x] = lane_roll(E[e, x, j], 8 + 16 * n)
                if w % 7 != 6:
                    put(U, N, PLACE[w], x, main_of(x, e, w))
        for x in planes:
            strips = E[strip_of(group), x, j]
            edges = jnp.zeros((8, 128), jnp.float32)
            for n, _m in members:
                edges = jnp.where(quarter_low == n, TMP[n, x], edges)
            for side, v in enumerate((jnp.where(third, edges, strips), jnp.where(third, strips, edges))):
                if group == DISPLACED:
                    held = lane_roll(v, -48) > 0.5
                    v = jnp.where((quarter_low % 4 == 0) & ~held, jnp.where(lane < 64, FAR, -FAR), v)
                LR[side, x] = v
        for x in planes:
            low, high = LR[0, x], LR[1, x]
            for n, _e, _w in fields:
                at = 32 * (x % 4) - 16 * n
                TMP[n, x] = jnp.where(quarter_low % 2 == 0, lane_roll(low, at), lane_roll(high, at + 16))
        for q, places in groups.items():
            for n, e, w in fields:
                f = PLACE[w]
                v = TMP[n, places[0]]
                for x in places[1:]:
                    v = jnp.where(segment == x % 4, TMP[n, x], v)
                HALO[f, q] = v
                put(U, N, f, 16 + q, v)
        for q, places in groups.items():
            for n, e, w in fields:
                f = PLACE[w]
                s = SENSE[f]
                if s:
                    v = HALO[f, q]
                    put(UZ, NZ, f, 16 + q, lane_roll(v, s))
                    put(XR, NR, f, q, lane_roll(v, 32 * s))
                    put(XZ, NX, f, q, lane_roll(v, 33 * s))
                    for x in places:
                        put(UZ, NZ, f, x, shifted(main_of(x, e, w), v, x % 4, s))

    def unpack_planes(group):
        for e in arrays_of(group):
            for i in range(2):
                v = RX[i, e]
                E[e, 10 + 2 * i, 0], E[e, 11 + 2 * i, 0] = v, swap(v)

    def unpack_corners(group):
        for e in arrays_of(group):
            for i in range(2):
                v = RC[i, e]
                E[e, 8 + 6 * i, 1], E[e, 9 + 6 * i, 1] = swap(v), v

    def before(x):
        return lax.rem(x + 15, 16)

    def after(x):
        return lax.rem(x + 1, 16)

    def group_at(q, n):
        return (q + n) % 4 if isinstance(q, int) else lax.rem(q + n, 4)

    def main_pair(f, x, oz):
        ref = UZ if oz else U
        return ref[f, x, 0], ref[f, x, 1]

    def halo_pair(f, q, ox, oz):
        if ox == 0:
            return main_pair(f, 16 + q, oz)
        ref = XZ if oz else XR
        s = SENSE[f]
        other = group_at(q, 3 if s > 0 else 1)
        return tuple(neighbour(ref[f, q, t], ref[f, other, t], s) for t in range(2))

    def bond_of(get, here, t, o):
        d = []
        for k in range(3):
            pair = get(D1 + k, o[0], o[2])
            v = below(pair, t) if o[1] else pair[t]
            d.append((v - here[k]) + (0.5 - o[k]))
        return d

    def bonds(get, unit):
        for t in range(2):
            here = [U[D0 + k, unit, t] for k in range(3)]
            for i, o in enumerate(corner_offsets):
                d = bond_of(get, here, t, o)
                r2 = d[0] * d[0] + d[1] * d[1] + d[2] * d[2]
                inverse = lax.rsqrt(r2)
                stretch = r2 * inverse - bond_length
                J[i, unit, t] = (0.25 * step_time * exchange_scale) * jnp.exp(-exchange_decay * stretch)
                P3[i, unit, t] = jnp.exp(-density_decay * stretch)
                RI[i, unit, t] = inverse

    def main_get(x):
        planes = (x, before(x))
        return lambda f, ox, oz: main_pair(f, planes[ox], oz)

    def halo_get(q):
        return lambda f, ox, oz: halo_pair(f, q, ox, oz)

    def main_bonds(x, _):
        bonds(main_get(x), x)
        return 0

    def halo_bonds(q, _):
        bonds(halo_get(q), 16 + q)
        return 0

    near, far, corner = tuple(range(8)), (8, 9, 10, 11, 13, 14, 15), (8, 9, 14, 15)
    halves(DISPLACED, near, 0)
    halves(SPUN, near, 0)
    for c in xs0:
        c.wait()
    unpack_planes(DISPLACED)
    halves(DISPLACED, far, 0)
    for c in xs1:
        c.wait()
    unpack_planes(SPUN)
    halves(SPUN, far, 0)
    for c in ys0:
        c.wait()
    for e in arrays_of(DISPLACED):
        unpack_rows(e)
    corners0 = corner_copies(28, DISPLACED)
    halves(DISPLACED, near, 1)
    lax.fori_loop(1, 8, main_bonds, 0)
    halo_bonds(1, 0)
    for c in ys1:
        c.wait()
    for e in arrays_of(SPUN):
        unpack_rows(e)
    corners1 = corner_copies(30, SPUN)
    for c in corners0:
        c.wait()
    unpack_corners(DISPLACED)
    halves(DISPLACED, corner, 1)
    main_bonds(0, 0)
    lax.fori_loop(8, 12, main_bonds, 0)
    lax.fori_loop(13, 16, main_bonds, 0)
    lax.fori_loop(2, 5, lambda n, c: halo_bonds(group_at(n, 0), c), 0)

    def halo_above(ref, i, q, ox, oz):
        if ox == 0:
            return [lane_roll(ref[i, 16 + q, t], -oz) if oz else ref[i, 16 + q, t] for t in range(2)]
        return [neighbour(lane_roll(ref[i, 16 + q, t], -32 - oz), lane_roll(ref[i, 16 + group_at(q, 1), t], -32 - oz), -1)
                for t in range(2)]

    def upper_bonds(q, _):
        following = group_at(q, 1)
        for i, o in enumerate(corner_offsets):
            pair = halo_above(J, i, q, o[0], o[2])
            for t in range(2):
                J1[i, 16 + q, t] = above(pair, t) if o[1] else pair[t]
            for p in range(4):
                n = p + o[0]
                x = 4 * q + n if n < 4 else 4 * following
                halo = 16 + (q if n < 4 else following)
                pair = [J[i, x, t] for t in range(2)]
                if o[2]:
                    pair = [shifted(pair[t], J[i, halo, t], n % 4, -1) for t in range(2)]
                for t in range(2):
                    J1[i, 4 * q + p, t] = above(pair, t) if o[1] else pair[t]
        return 0

    for q in range(4):
        upper_bonds(q, 0)

    halves(SPUN, near, 1)

    def slope(rho):
        return -0.5 * lax.rsqrt(1.0 + rho)

    def slopes(q, places):
        following = group_at(q, 1)
        if q < 3:
            for unit in [16 + q] + [4 * q + p for p in places]:
                for t in range(2):
                    F0[unit, t] = slope(functools.reduce(jnp.add, [P3[i, unit, t] for i in range(8)]))
        high = []
        rows = []
        for oy in range(2):
            far = [halo_above(P3, 4 + 2 * oy + oz, q, 1, 0) for oz in range(2)]
            flat = [P3[2 * oy, 16 + q, t] + far[0][t] for t in range(2)]
            high.append([P3[2 * oy + 1, 16 + q, t] + far[1][t] for t in range(2)])
            rows.append([flat[t] + lane_roll(high[oy][t], -1) for t in range(2)])
        halo = [slope(rows[0][t] + above(rows[1], t)) for t in range(2)]
        for t in range(2):
            spread(FS, q, t, halo[t], 1)
        for p in places:
            x = 4 * q + p
            x1 = 4 * q + p + 1 if p < 3 else 4 * following
            rows = []
            for oy in range(2):
                total = []
                for t in range(2):
                    flat = P3[2 * oy, x, t] + P3[4 + 2 * oy, x1, t]
                    top = P3[2 * oy + 1, x, t] + P3[5 + 2 * oy, x1, t]
                    total.append(flat + shifted(top, high[oy][t], p, -1))
                rows.append(total)
            for t in range(2):
                v = slope(rows[0][t] + above(rows[1], t))
                U[FS, x, t] = v
                UZ[FS, x, t] = shifted(v, halo[t], p, 1)

    for q, places in ((3, (3,)), (0, range(4)), (1, range(4)), (2, (0,))):
        slopes(q, places)

    for c in corners1:
        c.wait()
    unpack_corners(SPUN)
    halves(SPUN, corner, 1)
    field_load.wait()
    outer = [(0.25 * step_time) * field[k] for k in range(3)]

    def cross(a, b):
        return [a[1] * b[2] - a[2] * b[1], a[2] * b[0] - a[0] * b[2], a[0] * b[1] - a[1] * b[0]]

    def update(u):
        sector = u if u < 8 else 14 - u
        sub, quarter = sector % 2, sector // 2
        tile = quarter // 2
        source, target, step = (S1, S0, -1) if sub == 0 else (S0, S1, 1)
        coupling = J if sub == 0 else J1
        planes = turned_planes()[u]
        shift = below if sub == 0 else above
        s_new = SENSE[target]

        @functools.cache
        def around(k, x):
            found = {}
            for oz in range(2):
                pair = main_pair(source + k, x % 16, oz)
                found[0, oz], found[1, oz] = pair[tile], shift(pair, tile)
            return found

        def turned(get, unit):
            c = [coupling[i, unit, tile] for i in range(8)]
            h = []
            for k in range(3):
                total = outer[k]
                for i, o in enumerate(corner_offsets):
                    total = total + c[i] * get(k, o)
                h.append(total + total if u == 7 else total)
            s = [U[target + k, unit, tile] for k in range(3)]
            once = cross(h, s)
            twice = cross(h, once)
            factor = 2.0 / (1.0 + (h[0] * h[0] + h[1] * h[1] + h[2] * h[2]))
            return [s[k] + factor * (once[k] + twice[k]) for k in range(3)]

        halos = {}
        for q in sorted({x % 16 // 4 for x in planes}):
            found = {}
            for k in range(3):
                for ox in range(2):
                    for oz in range(2):
                        pair = halo_pair(source + k, q, ox, oz)
                        found[k, ox, 0, oz], found[k, ox, 1, oz] = pair[tile], shift(pair, tile)
            halos[q] = turned(lambda k, o: found[k, o[0], o[1], o[2]], 16 + q)
            for k in range(3):
                spread(target + k, q, tile, halos[q][k], s_new)
        for x in planes:
            unit = x % 16
            v = turned(lambda k, o: around(k, x + step * o[0])[o[1], o[2]], unit)
            for k in range(3):
                U[target + k, unit, tile] = v[k]
                UZ[target + k, unit, tile] = shifted(v[k], halos[unit // 4][k], unit % 4, s_new)

    for u in range(15):
        update(u)

    def strength(get, unit, t, i, o, here, spins, mine):
        d = bond_of(get, here, t, o)

        def at(f):
            pair = get(f, o[0], o[2])
            return below(pair, t) if o[1] else pair[t]

        align = functools.reduce(jnp.add, [spins[k] * at(S1 + k) for k in range(3)])
        p = P3[i, unit, t]
        g = (-density_decay * p * (p * (pair_decay * pair_scale / density_decay) + (mine + at(FS)))
             + (exchange_decay / (0.25 * step_time)) * J[i, unit, t] * align) * RI[i, unit, t]
        return [g * d[k] for k in range(3)]

    def of_unit(unit, t):
        return [U[D0 + k, unit, t] for k in range(3)], [U[S0 + k, unit, t] for k in range(3)], F0[unit, t]

    def halo_forces(q, _):
        for t in range(2):
            own = of_unit(16 + q, t)
            for i, o in enumerate(corner_offsets):
                if o[2]:
                    v = strength(halo_get(q), 16 + q, t, i, o, *own)
                    for k in range(3):
                        HP[i // 2, k, q, t] = v[k]
        return 0

    lax.fori_loop(0, 3, halo_forces, 0)

    def forces(x, q, p):
        planes = (x, before(x))
        sums = [[None] * 2 for _ in range(3)]
        parts = {}
        for t in range(2):
            own = of_unit(x, t)
            for i, o in enumerate(corner_offsets):
                v = strength(main_get(x), x, t, i, o, *own)
                for k in range(3):
                    parts[i, t, k] = v[k]
                    sums[k][t] = v[k] if sums[k][t] is None else sums[k][t] + v[k]
        for k in range(3):
            for t in range(2):
                ACC[k, x, t] = sums[k][t]
            for ox in range(2):
                rows = [[parts[4 * ox + 2 * oy, t, k] + shifted(parts[4 * ox + 2 * oy + 1, t, k], HP[2 * ox + oy, k, q, t], p, -1) for t in range(2)]
                        for oy in range(2)]
                for t in range(2):
                    v = rows[0][t] + above(rows[1], t)
                    if ox == 0:
                        ACC[3 + k, x, t] = -v
                    else:
                        ACC[3 + k, planes[1], t] = ACC[3 + k, planes[1], t] - v

    def four_forces(q, _):
        for p in range(4):
            forces(4 * q + p, q, p)
        return 0

    lax.fori_loop(0, 2, four_forces, 0)
    forces(8, 2, 0)

    def write(x, _):
        for f in range(6):
            for ref, at, out in ((U, (S1 if f > 2 else S0) + f % 3, out_s), (ACC, f, out_f)):
                out[f // 3, f % 3, x] = jnp.where(upper, ref[at, x, 0], ref[at, x, 1])
        return 0

    lax.fori_loop(0, 8, write, 0, unroll=4)


def emit(spins, forces, out_s, out_f, sem):
    copies = [pltpu.make_async_copy(a, b, sem.at[i]) for i, (a, b) in enumerate(((spins, out_s), (forces, out_f)))]
    for c in copies:
        c.start()
    for c in copies:
        c.wait()


def on_device(sizes, spin_vectors, displacement, occupied, applied_field):
    vmem = pl.BlockSpec(memory_space=pltpu.VMEM)
    hbm = pl.BlockSpec(memory_space=pltpu.HBM)
    shape = jax.ShapeDtypeStruct(spin_vectors.shape, jnp.float32)

    def buffer(*lead):
        return pltpu.VMEM(lead + (8, 128), jnp.float32)

    results = pl.pallas_call(
        functools.partial(kernel, sizes),
        out_shape=(pltpu.VMEM(shape.shape, jnp.float32),) * 2,
        in_specs=[hbm, hbm, hbm, hbm],
        out_specs=(vmem, vmem),
        scratch_shapes=[
            buffer(ARRAYS, 16, 2),
            buffer(2, 8), buffer(2, 2, 8),
            buffer(UP[-1]), buffer(UP[-1]),
            buffer(DOWN[-1]), buffer(DOWN[-1]),
            buffer(2, ARRAYS), buffer(2, ARRAYS),
            buffer(2, ARRAYS), buffer(2, ARRAYS),
            buffer(13, 20, 2), buffer(13, 20, 2), buffer(13, 4, 2), buffer(13, 4, 2), buffer(12, 20), buffer(12, 20), buffer(12, 4), buffer(12, 4), buffer(12, 4), buffer(2, 16), buffer(8, 16),
            buffer(8, 20, 2), buffer(8, 20, 2), buffer(8, 20, 2), buffer(8, 20, 2),
            buffer(20, 2), buffer(4, 3, 4, 2), buffer(6, 16, 2),
            pltpu.VMEM(spin_vectors.shape, jnp.float32),
            pltpu.VMEM(displacement.shape, jnp.float32),
            pltpu.VMEM(occupied.shape, jnp.int32),
            pltpu.SMEM(applied_field.shape, jnp.float32),
            pltpu.SemaphoreType.DMA((34,)),
            pltpu.SemaphoreType.DMA((34,)),
            pltpu.SemaphoreType.DMA((4,)),
        ],
        compiler_params=pltpu.CompilerParams(
            collective_id=0, has_side_effects=True, vmem_limit_bytes=60 * 1024 * 1024),
    )(spin_vectors, displacement, occupied, applied_field)
    return pl.pallas_call(
        emit,
        out_shape=(shape, shape),
        in_specs=[vmem, vmem],
        out_specs=(hbm, hbm),
        scratch_shapes=[pltpu.SemaphoreType.DMA((2,))],
        compiler_params=pltpu.CompilerParams(vmem_limit_bytes=4 * 1024 * 1024),
    )(*results)


def solution(mesh):
    sizes = tuple(mesh.shape[a] for a in axes)
    block = P(None, None, "gx", "gy", "gz")
    return jax.shard_map(
        functools.partial(on_device, sizes),
        mesh=mesh,
        in_specs=(block, block, P(None, "gx", "gy", "gz"), P()),
        out_specs=(block, block),
        check_vma=False,
    )
```

```python
import functools
import itertools

import jax
import jax.numpy as jnp
from jax import lax
from jax.experimental import pallas as pl
from jax.experimental.pallas import tpu as pltpu
from jax.sharding import PartitionSpec as P

step_time = 0.6
exchange_scale = 0.35
exchange_decay = 4.0
pair_scale = 0.5
pair_decay = 6.0
density_decay = 3.0
bond_length = 0.8660254037844386
corner_offsets = list(itertools.product((0, 1), repeat=3))
axes = ("gx", "gy", "gz")
MESH = pl.DeviceIdType.MESH

DISPLACED, SPUN = 0, 1
GROUPS = ((0, 4), (9, 3))
ARRAYS = 16
S0, D0, S1, D1, FS = 0, 3, 6, 9, 12
PLACE = {w: w - w // 7 for w in range(14) if w % 7 != 6}
SENSE = (-1,) * 3 + (0,) * 3 + (1,) * 7
FAR = 1000.0


def fields_of(group):
    first, n = GROUPS[group]
    return [(first + n * s + f, 7 * s + f + (3 if group == DISPLACED else 0), s) for s in range(2) for f in range(n)]


def strip_of(group):
    first, n = GROUPS[group]
    return first + 2 * n


TO_BELOW = tuple(
    [(i // 4, i, 0, 2, 2 * (i % 4)) for i in range(8)] + [(2, 2 + i, 2, 2, 2 * i) for i in range(4)])
TO_ABOVE_0 = tuple([(0, i, 7, 1, i) for i in range(8)] + [(1, 2 + i, 5, 2, 2 * i) for i in range(4)])
TO_ABOVE_1 = tuple(
    [(i // 4, i, 6, 2, 2 * (i % 4)) for i in range(8)] + [(2, 2 + i, 4, 2, 2 * i) for i in range(4)])


@functools.cache
def turned_planes():
    need = {(0, x, y) for x in range(9) for y in range(9)} | {(1, x, y) for x in range(-1, 8) for y in range(-1, 8)}
    need |= {(b, x, y) for b in (0, 1) for x in range(8) for y in range(8)}
    planes = {}
    for u in reversed(range(15)):
        sector = u if u < 8 else 14 - u
        sub, quarter = sector % 2, sector // 2
        turned = [k for k in need if k[0] == sub and k[1] // 4 % 2 + 2 * (k[2] // 4 % 2) == quarter]
        planes[u] = sorted({k[1] for k in turned})
        for _, x, y in turned:
            for a, b, _ in corner_offsets:
                need.add((1, x - a, y - b) if sub == 0 else (0, x + a, y + b))
    return planes


def working():
    rows = 8
    row = lax.broadcasted_iota(jnp.int32, (rows, 128), 0)
    first, last = row % 4 == 0, row % 4 == 3

    def turn(v, n):
        return pltpu.roll(v, n % rows, 0)

    def below(pair, tile):
        a, b = pair
        if tile == 0:
            return jnp.where(first, turn(b, 5), turn(a, 1))
        return jnp.where(first, turn(a, 1), turn(b, 1))

    def above(pair, tile):
        a, b = pair
        if tile == 0:
            return jnp.where(last, turn(b, -1), turn(a, -1))
        return jnp.where(last, turn(a, 3), turn(b, -1))

    return below, above


def place_rows():
    up, down, at, n_up, n_down = [], [], [], 0, 0
    for group in (DISPLACED, SPUN):
        for s in [s for _, _, s in fields_of(group)] + [1]:
            up.append(n_up)
            down.append(n_down)
            at.append(s)
            n_up += 2 + s
            n_down += 3
    return up + [n_up], down + [n_down], at


UP, DOWN, GEOMETRY = place_rows()


def kernel(sizes, spin_in, disp_in, occ_in, field_in, out_s, out_f, E, PZ, RZ, SU, RU, SD, RD, SX, RX, SC, RC, U, UZ, XR, XZ, N, NZ, NR, NX, HALO, LR, TMP, J, J1, P3, RI,
           F0, HP, ACC, spin, disp, occ, field, send_sem, recv_sem, load_sem):
    nx, ny, nz = sizes
    me = {a: lax.axis_index(a) for a in axes}
    count = dict(zip(axes, sizes))

    def peer(axis, step):
        n = count[axis]
        return {axis: lax.rem(me[axis] + (n + step), n)}

    peers = []
    for axis in axes:
        peers.append(peer(axis, 1))
        if count[axis] > 2:
            peers.append(peer(axis, -1))
    barrier = pltpu.get_barrier_semaphore()
    for p in peers:
        pl.semaphore_signal(barrier, inc=1, device_id=p, device_id_type=MESH)

    loads = [pltpu.make_async_copy(a, b, load_sem.at[i])
             for i, (a, b) in enumerate(((disp_in, disp), (occ_in, occ), (spin_in, spin)))]
    for c in loads:
        c.start()
    field_load = pltpu.make_async_copy(field_in, field, load_sem.at[3])
    field_load.start()

    lane = lax.broadcasted_iota(jnp.int32, (8, 128), 1)
    row = lax.broadcasted_iota(jnp.int32, (8, 128), 0)
    upper = row < 4

    def swap(v):
        return pltpu.roll(v, 4, 0)

    def load_own(group):
        for e, w, s in fields_of(group):
            f = w % 7
            for x in range(8):
                if f < 3:
                    E[e, x, 0] = spin[s, f, x]
                elif f < 6:
                    E[e, x, 0] = disp[s, f - 3, x]
                else:
                    E[e, x, 0] = occ[s, x].astype(jnp.float32)

    def pack_edges(group):
        for x in range(8):
            packed = jnp.zeros((8, 128), jnp.float32)
            for n, (e, w, s) in enumerate(fields_of(group)):
                packed = jnp.where(lane // 16 == n, pltpu.roll(E[e, x, 0], (8 + 16 * n) % 128, 1), packed)
            PZ[group, x] = packed

    inner = (row >= 2) & (row < 6)

    def routes(e):
        return ((SU, RU, UP[e], (TO_ABOVE_0, TO_ABOVE_1)[GEOMETRY[e]]), (SD, RD, DOWN[e], TO_BELOW))

    def pack_rows(e):
        own = [E[e, x, 0] for x in range(8)]
        for out, _unused, first, pieces in routes(e):
            tiles = {}
            for tile, x, low, n, to in pieces:
                v = pltpu.roll(own[x], (to - low) % 8, 0)
                tiles[tile] = jnp.where(row < to, tiles[tile], v) if to else v
            for tile, v in tiles.items():
                out[first + tile] = v
        SX[0, e] = jnp.where(inner, own[2], swap(own[3]))
        SX[1, e] = jnp.where(inner, own[4], swap(own[5]))

    def unpack_rows(e):
        rows = [jnp.zeros((8, 128), jnp.float32)] * 8
        for _unused, arrived, first, pieces in routes(e):
            for tile, x, low, n, to in pieces:
                v = pltpu.roll(arrived[first + tile], (low - to) % 8, 0)
                rows[x] = jnp.where((row >= low) & (row < low + n), v, rows[x])
        for x in range(8):
            E[e, x, 1] = swap(rows[x])
        SC[0, e] = jnp.where(inner, swap(rows[1]), rows[0])
        SC[1, e] = jnp.where(inner, swap(rows[7]), rows[6])

    def arrays_of(group):
        return range(GROUPS[group][0], strip_of(group) + 1)

    def send(i, src, dst, to):
        c = pltpu.make_async_remote_copy(
            src_ref=src, dst_ref=dst, send_sem=send_sem.at[i], recv_sem=recv_sem.at[i],
            device_id=to, device_id_type=MESH)
        c.start()
        return c

    def exchange_y(i, lo, hi):
        up = pl.ds(UP[lo], UP[hi] - UP[lo])
        down = pl.ds(DOWN[lo], DOWN[hi] - DOWN[lo])
        return [
            send(i, SD.at[down], RD.at[down], peer("gy", -1)),
            send(i + 1, SU.at[up], RU.at[up], peer("gy", 1)),
        ]

    def exchange_x(i, lo, hi):
        part = pl.ds(lo, hi - lo)

        def plane(x):
            return E.at[part, pl.ds(x, 2), 0]

        return [
            send(i, plane(0), plane(8), peer("gx", -1)),
            send(i + 1, plane(6), plane(14), peer("gx", 1)),
            send(i + 2, SX.at[0, part], RX.at[0, part], peer("gx", -1)),
            send(i + 3, SX.at[1, part], RX.at[1, part], peer("gx", 1)),
        ]

    def exchange_z(i, group):
        found = [send(i, PZ.at[group], RZ.at[0, group], peer("gz", -1))]
        if nz > 2:
            found.append(send(i + 1, PZ.at[group], RZ.at[1, group], peer("gz", 1)))
        return found

    def take_strips(group, copies):
        for c in copies:
            c.wait()
        for x in range(8):
            v = RZ[0, group, x]
            if nz > 2:
                v = jnp.where(lane % 16 < 8, RZ[1, group, x], v)
            E[strip_of(group), x, 0] = v
        pack_rows(strip_of(group))

    def corner_copies(i, group):
        part = pl.ds(GROUPS[group][0], len(arrays_of(group)))
        return [send(i + n, SC.at[n, part], RC.at[n, part], peer("gx", 2 * n - 1)) for n in range(2)]

    loads[0].wait()
    loads[1].wait()
    load_own(DISPLACED)
    for e, _, _ in fields_of(DISPLACED):
        pack_rows(e)
    pack_edges(DISPLACED)
    loads[2].wait()
    load_own(SPUN)
    for e, _, _ in fields_of(SPUN):
        pack_rows(e)
    pack_edges(SPUN)
    pl.semaphore_wait(barrier, len(peers))
    z0 = exchange_z(0, DISPLACED)
    ys0 = exchange_y(4, GROUPS[0][0], strip_of(0))
    z1 = exchange_z(2, SPUN)
    ys1 = exchange_y(8, GROUPS[1][0], GROUPS[1][0] + 1)
    xs0 = exchange_x(12, GROUPS[0][0], strip_of(0))
    take_strips(DISPLACED, z0)
    ys0 += exchange_y(6, strip_of(0), strip_of(0) + 1)
    ys1 += exchange_y(32, GROUPS[1][0] + 1, strip_of(1))
    xs0 += exchange_x(16, strip_of(0), strip_of(0) + 1)
    xs1 = exchange_x(20, GROUPS[1][0], strip_of(1))
    take_strips(SPUN, z1)
    ys1 += exchange_y(10, strip_of(1), strip_of(1) + 1)
    xs1 += exchange_x(24, strip_of(1), strip_of(1) + 1)

    below, above = working()
    segment = lane // 32
    third, quarter_low = lane % 16 >= 8, lane // 16

    def lane_roll(v, n):
        return pltpu.roll(v, n % 128, 1)

    def edge_of(halo, p, s):
        return lane_roll(halo, -(32 * p + 7) if s > 0 else 103 - 32 * p)

    def shifted(main, halo, p, s):
        return jnp.where(lane == (0 if s > 0 else 127), edge_of(halo, p, s), lane_roll(main, s))

    def spread(f, q, t, halo, s):
        U[f, 16 + q, t] = halo
        UZ[f, 16 + q, t] = lane_roll(halo, s)
        XR[f, q, t] = lane_roll(halo, 32 * s)
        XZ[f, q, t] = lane_roll(halo, 33 * s)

    def neighbour(now, other, s):
        return jnp.where(segment == (0 if s > 0 else 3), other, now)

    def halves(group, planes, j):
        fields = [(n, e, w) for n, (e, w, s) in enumerate(fields_of(group)) if w % 7 != 6]
        members = list(enumerate(fields_of(group)))
        groups = {}
        for x in planes:
            groups.setdefault(x // 4, []).append(x)
        lone = range(10, 14)

        def put(ref, kept, f, unit, v):
            if j == 0 and unit in lone:
                ref[f, unit, 0], ref[f, unit, 1] = v, v
            elif j == 0:
                kept[f, unit] = v
                if unit in (8, 9, 14, 15):
                    ref[f, unit, 0], ref[f, unit, 1] = v, v
            else:
                own = kept[f, unit]
                ref[f, unit, 0], ref[f, unit, 1] = jnp.where(upper, own, v), jnp.where(upper, v, own)

        def main_of(x, e, w):
            if w % 7 == 3:
                return jnp.where(E[e + 3, x, j] > 0.5, E[e, x, j], FAR if w < 7 else -FAR)
            return E[e, x, j]

        for x in planes:
            for n, (e, w, _s) in members:
                TMP[n, x] = lane_roll(E[e, x, j], 8 + 16 * n)
                if w % 7 != 6:
                    put(U, N, PLACE[w], x, main_of(x, e, w))
        for x in planes:
            strips = E[strip_of(group), x, j]
            edges = jnp.zeros((8, 128), jnp.float32)
            for n, _m in members:
                edges = jnp.where(quarter_low == n, TMP[n, x], edges)
            for side, v in enumerate((jnp.where(third, edges, strips), jnp.where(third, strips, edges))):
                if group == DISPLACED:
                    held = lane_roll(v, -48) > 0.5
                    v = jnp.where((quarter_low % 4 == 0) & ~held, jnp.where(lane < 64, FAR, -FAR), v)
                LR[side, x] = v
        for x in planes:
            low, high = LR[0, x], LR[1, x]
            for n, _e, _w in fields:
                at = 32 * (x % 4) - 16 * n
                TMP[n, x] = jnp.where(quarter_low % 2 == 0, lane_roll(low, at), lane_roll(high, at + 16))
        for q, places in groups.items():
            for n, e, w in fields:
                f = PLACE[w]
                v = TMP[n, places[0]]
                for x in places[1:]:
                    v = jnp.where(segment == x % 4, TMP[n, x], v)
                HALO[f, q] = v
                put(U, N, f, 16 + q, v)
        for q, places in groups.items():
            for n, e, w in fields:
                f = PLACE[w]
                s = SENSE[f]
                if s:
                    v = HALO[f, q]
                    put(UZ, NZ, f, 16 + q, lane_roll(v, s))
                    put(XR, NR, f, q, lane_roll(v, 32 * s))
                    put(XZ, NX, f, q, lane_roll(v, 33 * s))
                    for x in places:
                        put(UZ, NZ, f, x, shifted(main_of(x, e, w), v, x % 4, s))

    def unpack_planes(group):
        for e in arrays_of(group):
            for i in range(2):
                v = RX[i, e]
                E[e, 10 + 2 * i, 0], E[e, 11 + 2 * i, 0] = v, swap(v)

    def unpack_corners(group):
        for e in arrays_of(group):
            for i in range(2):
                v = RC[i, e]
                E[e, 8 + 6 * i, 1], E[e, 9 + 6 * i, 1] = swap(v), v

    def before(x):
        return lax.rem(x + 15, 16)

    def after(x):
        return lax.rem(x + 1, 16)

    def group_at(q, n):
        return (q + n) % 4 if isinstance(q, int) else lax.rem(q + n, 4)

    def main_pair(f, x, oz):
        ref = UZ if oz else U
        return ref[f, x, 0], ref[f, x, 1]

    def halo_pair(f, q, ox, oz):
        if ox == 0:
            return main_pair(f, 16 + q, oz)
        ref = XZ if oz else XR
        s = SENSE[f]
        other = group_at(q, 3 if s > 0 else 1)
        return tuple(neighbour(ref[f, q, t], ref[f, other, t], s) for t in range(2))

    def bond_of(get, here, t, o):
        d = []
        for k in range(3):
            pair = get(D1 + k, o[0], o[2])
            v = below(pair, t) if o[1] else pair[t]
            d.append((v - here[k]) + (0.5 - o[k]))
        return d

    def bonds(get, unit, crossing=False):
        for t in range(2):
            here = [U[D0 + k, unit, t] for k in range(3)]
            for i, o in enumerate(corner_offsets):
                if crossing and not o[0]:
                    continue
                d = bond_of(get, here, t, o)
                r2 = d[0] * d[0] + d[1] * d[1] + d[2] * d[2]
                inverse = lax.rsqrt(r2)
                stretch = r2 * inverse - bond_length
                J[i, unit, t] = (0.25 * step_time * exchange_scale) * jnp.exp(-exchange_decay * stretch)
                P3[i, unit, t] = jnp.exp(-density_decay * stretch)
                RI[i, unit, t] = inverse

    def main_get(x):
        planes = (x, before(x))
        return lambda f, ox, oz: main_pair(f, planes[ox], oz)

    def halo_get(q):
        return lambda f, ox, oz: halo_pair(f, q, ox, oz)

    def main_bonds(x, _):
        bonds(main_get(x), x)
        return 0

    def halo_bonds(q, _):
        bonds(halo_get(q), 16 + q)
        return 0

    def halo_above(ref, i, q, ox, oz):
        if ox == 0:
            return [lane_roll(ref[i, 16 + q, t], -oz) if oz else ref[i, 16 + q, t] for t in range(2)]
        return [neighbour(lane_roll(ref[i, 16 + q, t], -32 - oz), lane_roll(ref[i, 16 + group_at(q, 1), t], -32 - oz), -1)
                for t in range(2)]

    def upper_bonds(q, _):
        following = group_at(q, 1)
        for i, o in enumerate(corner_offsets):
            pair = halo_above(J, i, q, o[0], o[2])
            for t in range(2):
                J1[i, 16 + q, t] = above(pair, t) if o[1] else pair[t]
            for p in [p for p in range(4) if 4 * q + p not in (11, 12)]:
                n = p + o[0]
                x = 4 * q + n if n < 4 else 4 * following
                halo = 16 + (q if n < 4 else following)
                pair = [J[i, x, t] for t in range(2)]
                if o[2]:
                    pair = [shifted(pair[t], J[i, halo, t], n % 4, -1) for t in range(2)]
                for t in range(2):
                    J1[i, 4 * q + p, t] = above(pair, t) if o[1] else pair[t]
        return 0

    def slope(rho):
        return -0.5 * lax.rsqrt(1.0 + rho)

    def own_slopes(units):
        for unit in units:
            for t in range(2):
                F0[unit, t] = slope(functools.reduce(jnp.add, [P3[i, unit, t] for i in range(8)]))

    def slopes(q, places):
        following = group_at(q, 1)
        high = []
        rows = []
        for oy in range(2):
            far = [halo_above(P3, 4 + 2 * oy + oz, q, 1, 0) for oz in range(2)]
            flat = [P3[2 * oy, 16 + q, t] + far[0][t] for t in range(2)]
            high.append([P3[2 * oy + 1, 16 + q, t] + far[1][t] for t in range(2)])
            rows.append([flat[t] + lane_roll(high[oy][t], -1) for t in range(2)])
        halo = [slope(rows[0][t] + above(rows[1], t)) for t in range(2)]
        for t in range(2):
            spread(FS, q, t, halo[t], 1)
        for p in places:
            x = 4 * q + p
            x1 = 4 * q + p + 1 if p < 3 else 4 * following
            rows = []
            for oy in range(2):
                total = []
                for t in range(2):
                    flat = P3[2 * oy, x, t] + P3[4 + 2 * oy, x1, t]
                    top = P3[2 * oy + 1, x, t] + P3[5 + 2 * oy, x1, t]
                    total.append(flat + shifted(top, high[oy][t], p, -1))
                rows.append(total)
            for t in range(2):
                v = slope(rows[0][t] + above(rows[1], t))
                U[FS, x, t] = v
                UZ[FS, x, t] = shifted(v, halo[t], p, 1)

    near, far, corner = tuple(range(8)), tuple(range(8, 16)), (8, 9, 14, 15)
    halves(DISPLACED, near, 0)
    halves(SPUN, near, 0)
    for c in xs0:
        c.wait()
    unpack_planes(DISPLACED)
    halves(DISPLACED, far, 0)
    for c in ys0:
        c.wait()
    for e in arrays_of(DISPLACED):
        unpack_rows(e)
    corners0 = corner_copies(28, DISPLACED)
    halves(DISPLACED, near, 1)
    lax.fori_loop(0, 8, main_bonds, 0)
    lax.fori_loop(0, 2, halo_bonds, 0)
    lax.fori_loop(10, 12, main_bonds, 0)
    main_bonds(13, 0)
    upper_bonds(0, 0)
    slopes(0, range(4))
    own_slopes((1, 2, 3, 4, 5, 6, 7, 17))
    for c in xs1:
        c.wait()
    unpack_planes(SPUN)
    halves(SPUN, far, 0)
    for c in ys1:
        c.wait()
    for e in arrays_of(SPUN):
        unpack_rows(e)
    corners1 = corner_copies(30, SPUN)
    halves(SPUN, near, 1)
    for c in corners0:
        c.wait()
    unpack_corners(DISPLACED)
    halves(DISPLACED, corner, 1)
    bonds(main_get(0), 0, True)
    lax.fori_loop(8, 10, main_bonds, 0)
    lax.fori_loop(14, 16, main_bonds, 0)
    lax.fori_loop(2, 5, lambda n, c: halo_bonds(group_at(n, 0), c), 0)
    for q in range(1, 4):
        upper_bonds(q, 0)
    for q, places in ((3, (3,)), (1, range(4)), (2, (0,))):
        slopes(q, places)
    own_slopes((0, 8, 16, 18))
    for c in corners1:
        c.wait()
    unpack_corners(SPUN)
    halves(SPUN, corner, 1)
    field_load.wait()
    outer = [(0.25 * step_time) * field[k] for k in range(3)]

    def cross(a, b):
        return [a[1] * b[2] - a[2] * b[1], a[2] * b[0] - a[0] * b[2], a[0] * b[1] - a[1] * b[0]]

    def update(u):
        sector = u if u < 8 else 14 - u
        sub, quarter = sector % 2, sector // 2
        tile = quarter // 2
        source, target, step = (S1, S0, -1) if sub == 0 else (S0, S1, 1)
        coupling = J if sub == 0 else J1
        planes = turned_planes()[u]
        shift = below if sub == 0 else above
        s_new = SENSE[target]

        @functools.cache
        def around(k, x):
            found = {}
            for oz in range(2):
                pair = main_pair(source + k, x % 16, oz)
                found[0, oz], found[1, oz] = pair[tile], shift(pair, tile)
            return found

        def turned(get, unit):
            c = [coupling[i, unit, tile] for i in range(8)]
            h = []
            for k in range(3):
                total = outer[k]
                for i, o in enumerate(corner_offsets):
                    total = total + c[i] * get(k, o)
                h.append(total + total if u == 7 else total)
            s = [U[target + k, unit, tile] for k in range(3)]
            once = cross(h, s)
            twice = cross(h, once)
            factor = 2.0 / (1.0 + (h[0] * h[0] + h[1] * h[1] + h[2] * h[2]))
            return [s[k] + factor * (once[k] + twice[k]) for k in range(3)]

        halos = {}
        for q in sorted({x % 16 // 4 for x in planes}):
            found = {}
            for k in range(3):
                for ox in range(2):
                    for oz in range(2):
                        pair = halo_pair(source + k, q, ox, oz)
                        found[k, ox, 0, oz], found[k, ox, 1, oz] = pair[tile], shift(pair, tile)
            halos[q] = turned(lambda k, o: found[k, o[0], o[1], o[2]], 16 + q)
            for k in range(3):
                spread(target + k, q, tile, halos[q][k], s_new)
        for x in planes:
            unit = x % 16
            v = turned(lambda k, o: around(k, x + step * o[0])[o[1], o[2]], unit)
            for k in range(3):
                U[target + k, unit, tile] = v[k]
                UZ[target + k, unit, tile] = shifted(v[k], halos[unit // 4][k], unit % 4, s_new)

    for u in range(15):
        update(u)

    def strength(get, unit, t, i, o, here, spins, mine):
        d = bond_of(get, here, t, o)

        def at(f):
            pair = get(f, o[0], o[2])
            return below(pair, t) if o[1] else pair[t]

        align = functools.reduce(jnp.add, [spins[k] * at(S1 + k) for k in range(3)])
        p = P3[i, unit, t]
        g = (-density_decay * p * (p * (pair_decay * pair_scale / density_decay) + (mine + at(FS)))
             + (exchange_decay / (0.25 * step_time)) * J[i, unit, t] * align) * RI[i, unit, t]
        return [g * d[k] for k in range(3)]

    def of_unit(unit, t):
        return [U[D0 + k, unit, t] for k in range(3)], [U[S0 + k, unit, t] for k in range(3)], F0[unit, t]

    def halo_forces(q, _):
        for t in range(2):
            own = of_unit(16 + q, t)
            for i, o in enumerate(corner_offsets):
                if o[2]:
                    v = strength(halo_get(q), 16 + q, t, i, o, *own)
                    for k in range(3):
                        HP[i // 2, k, q, t] = v[k]
        return 0

    lax.fori_loop(0, 3, halo_forces, 0)

    def forces(x, q, p):
        planes = (x, before(x))
        sums = [[None] * 2 for _ in range(3)]
        parts = {}
        for t in range(2):
            own = of_unit(x, t)
            for i, o in enumerate(corner_offsets):
                v = strength(main_get(x), x, t, i, o, *own)
                for k in range(3):
                    parts[i, t, k] = v[k]
                    sums[k][t] = v[k] if sums[k][t] is None else sums[k][t] + v[k]
        for k in range(3):
            for t in range(2):
                ACC[k, x, t] = sums[k][t]
            for ox in range(2):
                rows = [[parts[4 * ox + 2 * oy, t, k] + shifted(parts[4 * ox + 2 * oy + 1, t, k], HP[2 * ox + oy, k, q, t], p, -1) for t in range(2)]
                        for oy in range(2)]
                for t in range(2):
                    v = rows[0][t] + above(rows[1], t)
                    if ox == 0:
                        ACC[3 + k, x, t] = -v
                    else:
                        ACC[3 + k, planes[1], t] = ACC[3 + k, planes[1], t] - v

    def four_forces(q, _):
        for p in range(4):
            forces(4 * q + p, q, p)
        return 0

    lax.fori_loop(0, 2, four_forces, 0)
    forces(8, 2, 0)

    def write(x, _):
        for f in range(6):
            for ref, at, out in ((U, (S1 if f > 2 else S0) + f % 3, out_s), (ACC, f, out_f)):
                out[f // 3, f % 3, x] = jnp.where(upper, ref[at, x, 0], ref[at, x, 1])
        return 0

    lax.fori_loop(0, 8, write, 0, unroll=4)


def emit(spins, forces, out_s, out_f, sem):
    copies = [pltpu.make_async_copy(a, b, sem.at[i]) for i, (a, b) in enumerate(((spins, out_s), (forces, out_f)))]
    for c in copies:
        c.start()
    for c in copies:
        c.wait()


def on_device(sizes, spin_vectors, displacement, occupied, applied_field):
    vmem = pl.BlockSpec(memory_space=pltpu.VMEM)
    hbm = pl.BlockSpec(memory_space=pltpu.HBM)
    shape = jax.ShapeDtypeStruct(spin_vectors.shape, jnp.float32)

    def buffer(*lead):
        return pltpu.VMEM(lead + (8, 128), jnp.float32)

    results = pl.pallas_call(
        functools.partial(kernel, sizes),
        out_shape=(pltpu.VMEM(shape.shape, jnp.float32),) * 2,
        in_specs=[hbm, hbm, hbm, hbm],
        out_specs=(vmem, vmem),
        scratch_shapes=[
            buffer(ARRAYS, 16, 2),
            buffer(2, 8), buffer(2, 2, 8),
            buffer(UP[-1]), buffer(UP[-1]),
            buffer(DOWN[-1]), buffer(DOWN[-1]),
            buffer(2, ARRAYS), buffer(2, ARRAYS),
            buffer(2, ARRAYS), buffer(2, ARRAYS),
            buffer(13, 20, 2), buffer(13, 20, 2), buffer(13, 4, 2), buffer(13, 4, 2), buffer(12, 20), buffer(12, 20), buffer(12, 4), buffer(12, 4), buffer(12, 4), buffer(2, 16), buffer(8, 16),
            buffer(8, 20, 2), buffer(8, 20, 2), buffer(8, 20, 2), buffer(8, 20, 2),
            buffer(20, 2), buffer(4, 3, 4, 2), buffer(6, 16, 2),
            pltpu.VMEM(spin_vectors.shape, jnp.float32),
            pltpu.VMEM(displacement.shape, jnp.float32),
            pltpu.VMEM(occupied.shape, jnp.int32),
            pltpu.SMEM(applied_field.shape, jnp.float32),
            pltpu.SemaphoreType.DMA((34,)),
            pltpu.SemaphoreType.DMA((34,)),
            pltpu.SemaphoreType.DMA((4,)),
        ],
        compiler_params=pltpu.CompilerParams(
            collective_id=0, has_side_effects=True, vmem_limit_bytes=60 * 1024 * 1024),
    )(spin_vectors, displacement, occupied, applied_field)
    return pl.pallas_call(
        emit,
        out_shape=(shape, shape),
        in_specs=[vmem, vmem],
        out_specs=(hbm, hbm),
        scratch_shapes=[pltpu.SemaphoreType.DMA((2,))],
        compiler_params=pltpu.CompilerParams(vmem_limit_bytes=4 * 1024 * 1024),
    )(*results)


def solution(mesh):
    sizes = tuple(mesh.shape[a] for a in axes)
    block = P(None, None, "gx", "gy", "gz")
    return jax.shard_map(
        functools.partial(on_device, sizes),
        mesh=mesh,
        in_specs=(block, block, P(None, "gx", "gy", "gz"), P()),
        out_specs=(block, block),
        check_vma=False,
    )
```

```python
import functools
import itertools

import jax
import jax.numpy as jnp
from jax import lax
from jax.experimental import pallas as pl
from jax.experimental.pallas import tpu as pltpu
from jax.sharding import PartitionSpec as P

step_time = 0.6
exchange_scale = 0.35
exchange_decay = 4.0
pair_scale = 0.5
pair_decay = 6.0
density_decay = 3.0
bond_length = 0.8660254037844386
corner_offsets = list(itertools.product((0, 1), repeat=3))
axes = ("gx", "gy", "gz")
MESH = pl.DeviceIdType.MESH

DISPLACED, SPUN = 0, 1
GROUPS = ((0, 4), (9, 3))
ARRAYS = 16
S0, D0, S1, D1, FS = 0, 3, 6, 9, 12
PLACE = {w: w - w // 7 for w in range(14) if w % 7 != 6}
SENSE = (-1,) * 3 + (0,) * 3 + (1,) * 7
FAR = 1000.0


def fields_of(group):
    first, n = GROUPS[group]
    return [(first + n * s + f, 7 * s + f + (3 if group == DISPLACED else 0), s) for s in range(2) for f in range(n)]


def strip_of(group):
    first, n = GROUPS[group]
    return first + 2 * n


TO_BELOW = tuple(
    [(i // 4, i, 0, 2, 2 * (i % 4)) for i in range(8)] + [(2, 2 + i, 2, 2, 2 * i) for i in range(4)])
TO_ABOVE_0 = tuple([(0, i, 7, 1, i) for i in range(8)] + [(1, 2 + i, 5, 2, 2 * i) for i in range(4)])
TO_ABOVE_1 = tuple(
    [(i // 4, i, 6, 2, 2 * (i % 4)) for i in range(8)] + [(2, 2 + i, 4, 2, 2 * i) for i in range(4)])


@functools.cache
def turned_planes():
    need = {(0, x, y) for x in range(9) for y in range(9)} | {(1, x, y) for x in range(-1, 8) for y in range(-1, 8)}
    need |= {(b, x, y) for b in (0, 1) for x in range(8) for y in range(8)}
    planes = {}
    for u in reversed(range(15)):
        sector = u if u < 8 else 14 - u
        sub, quarter = sector % 2, sector // 2
        turned = [k for k in need if k[0] == sub and k[1] // 4 % 2 + 2 * (k[2] // 4 % 2) == quarter]
        planes[u] = sorted({k[1] for k in turned})
        for _, x, y in turned:
            for a, b, _ in corner_offsets:
                need.add((1, x - a, y - b) if sub == 0 else (0, x + a, y + b))
    return planes


def working():
    rows = 8
    row = lax.broadcasted_iota(jnp.int32, (rows, 128), 0)
    first, last = row % 4 == 0, row % 4 == 3

    def turn(v, n):
        return pltpu.roll(v, n % rows, 0)

    def below(pair, tile):
        a, b = pair
        if tile == 0:
            return jnp.where(first, turn(b, 5), turn(a, 1))
        return jnp.where(first, turn(a, 1), turn(b, 1))

    def above(pair, tile):
        a, b = pair
        if tile == 0:
            return jnp.where(last, turn(b, -1), turn(a, -1))
        return jnp.where(last, turn(a, 3), turn(b, -1))

    return below, above


def place_rows():
    up, down, at, n_up, n_down = [], [], [], 0, 0
    for group in (DISPLACED, SPUN):
        for s in [s for _, _, s in fields_of(group)] + [1]:
            up.append(n_up)
            down.append(n_down)
            at.append(s)
            n_up += 2 + s
            n_down += 3
    return up + [n_up], down + [n_down], at


UP, DOWN, GEOMETRY = place_rows()


def kernel(sizes, spin_in, disp_in, occ_in, field_in, out_s, out_f, E, PZ, RZ, SU, RU, SD, RD, SX, RX, SC, RC, U, UZ, XR, XZ, N, NZ, NR, NX, HALO, LR, TMP, J, J1, P3, RI,
           F0, HP, ACC, spin, disp, occ, field, send_sem, recv_sem, load_sem):
    nx, ny, nz = sizes
    me = {a: lax.axis_index(a) for a in axes}
    count = dict(zip(axes, sizes))

    def peer(axis, step):
        n = count[axis]
        return {axis: lax.rem(me[axis] + (n + step), n)}

    peers = []
    for axis in axes:
        peers.append(peer(axis, 1))
        if count[axis] > 2:
            peers.append(peer(axis, -1))
    barrier = pltpu.get_barrier_semaphore()
    for p in peers:
        pl.semaphore_signal(barrier, inc=1, device_id=p, device_id_type=MESH)

    loads = [pltpu.make_async_copy(a, b, load_sem.at[i])
             for i, (a, b) in enumerate(((disp_in, disp), (occ_in, occ), (spin_in, spin)))]
    for c in loads:
        c.start()
    field_load = pltpu.make_async_copy(field_in, field, load_sem.at[3])
    field_load.start()

    lane = lax.broadcasted_iota(jnp.int32, (8, 128), 1)
    row = lax.broadcasted_iota(jnp.int32, (8, 128), 0)
    upper = row < 4

    def swap(v):
        return pltpu.roll(v, 4, 0)

    def load_own(group):
        for e, w, s in fields_of(group):
            f = w % 7
            for x in range(8):
                if f < 3:
                    E[e, x, 0] = spin[s, f, x]
                elif f < 6:
                    E[e, x, 0] = disp[s, f - 3, x]
                else:
                    E[e, x, 0] = occ[s, x].astype(jnp.float32)

    def pack_edges(group):
        for x in range(8):
            packed = jnp.zeros((8, 128), jnp.float32)
            for n, (e, w, s) in enumerate(fields_of(group)):
                packed = jnp.where(lane // 16 == n, pltpu.roll(E[e, x, 0], (8 + 16 * n) % 128, 1), packed)
            PZ[group, x] = packed

    inner = (row >= 2) & (row < 6)

    def routes(e):
        return ((SU, RU, UP[e], (TO_ABOVE_0, TO_ABOVE_1)[GEOMETRY[e]]), (SD, RD, DOWN[e], TO_BELOW))

    def pack_rows(e):
        own = [E[e, x, 0] for x in range(8)]
        for out, _unused, first, pieces in routes(e):
            tiles = {}
            for tile, x, low, n, to in pieces:
                v = pltpu.roll(own[x], (to - low) % 8, 0)
                tiles[tile] = jnp.where(row < to, tiles[tile], v) if to else v
            for tile, v in tiles.items():
                out[first + tile] = v
        SX[0, e] = jnp.where(inner, own[2], swap(own[3]))
        SX[1, e] = jnp.where(inner, own[4], swap(own[5]))

    def unpack_rows(e):
        rows = [jnp.zeros((8, 128), jnp.float32)] * 8
        for _unused, arrived, first, pieces in routes(e):
            for tile, x, low, n, to in pieces:
                v = pltpu.roll(arrived[first + tile], (low - to) % 8, 0)
                rows[x] = jnp.where((row >= low) & (row < low + n), v, rows[x])
        for x in range(8):
            E[e, x, 1] = swap(rows[x])
        SC[0, e] = jnp.where(inner, swap(rows[1]), rows[0])
        SC[1, e] = jnp.where(inner, swap(rows[7]), rows[6])

    def arrays_of(group):
        return range(GROUPS[group][0], strip_of(group) + 1)

    def send(i, src, dst, to):
        c = pltpu.make_async_remote_copy(
            src_ref=src, dst_ref=dst, send_sem=send_sem.at[i], recv_sem=recv_sem.at[i],
            device_id=to, device_id_type=MESH)
        c.start()
        return c

    def exchange_y(i, lo, hi):
        up = pl.ds(UP[lo], UP[hi] - UP[lo])
        down = pl.ds(DOWN[lo], DOWN[hi] - DOWN[lo])
        return [
            send(i, SD.at[down], RD.at[down], peer("gy", -1)),
            send(i + 1, SU.at[up], RU.at[up], peer("gy", 1)),
        ]

    def exchange_x(i, lo, hi):
        part = pl.ds(lo, hi - lo)

        def plane(x):
            return E.at[part, pl.ds(x, 2), 0]

        return [
            send(i, plane(0), plane(8), peer("gx", -1)),
            send(i + 1, plane(6), plane(14), peer("gx", 1)),
            send(i + 2, SX.at[0, part], RX.at[0, part], peer("gx", -1)),
            send(i + 3, SX.at[1, part], RX.at[1, part], peer("gx", 1)),
        ]

    def exchange_z(i, group):
        found = [send(i, PZ.at[group], RZ.at[0, group], peer("gz", -1))]
        if nz > 2:
            found.append(send(i + 1, PZ.at[group], RZ.at[1, group], peer("gz", 1)))
        return found

    def take_strips(group, copies):
        for c in copies:
            c.wait()
        for x in range(8):
            v = RZ[0, group, x]
            if nz > 2:
                v = jnp.where(lane % 16 < 8, RZ[1, group, x], v)
            E[strip_of(group), x, 0] = v
        pack_rows(strip_of(group))

    def corner_copies(i, group):
        part = pl.ds(GROUPS[group][0], len(arrays_of(group)))
        return [send(i + n, SC.at[n, part], RC.at[n, part], peer("gx", 2 * n - 1)) for n in range(2)]

    loads[0].wait()
    loads[1].wait()
    load_own(DISPLACED)
    for e, _, _ in fields_of(DISPLACED):
        pack_rows(e)
    pl.semaphore_wait(barrier, len(peers))
    ys0 = exchange_y(4, GROUPS[0][0], strip_of(0))
    pack_edges(DISPLACED)
    z0 = exchange_z(0, DISPLACED)
    loads[2].wait()
    load_own(SPUN)
    for e, _, _ in fields_of(SPUN):
        pack_rows(e)
    ys1 = exchange_y(8, GROUPS[1][0], GROUPS[1][0] + 1)
    pack_edges(SPUN)
    z1 = exchange_z(2, SPUN)
    xs0 = exchange_x(12, GROUPS[0][0], strip_of(0))
    xs1 = exchange_x(20, GROUPS[1][0], strip_of(1))
    take_strips(DISPLACED, z0)
    ys0 += exchange_y(6, strip_of(0), strip_of(0) + 1)
    ys1 += exchange_y(32, GROUPS[1][0] + 1, strip_of(1))
    xs0 += exchange_x(16, strip_of(0), strip_of(0) + 1)
    take_strips(SPUN, z1)
    ys1 += exchange_y(10, strip_of(1), strip_of(1) + 1)
    xs1 += exchange_x(24, strip_of(1), strip_of(1) + 1)

    below, above = working()
    segment = lane // 32
    third, quarter_low = lane % 16 >= 8, lane // 16

    def lane_roll(v, n):
        return pltpu.roll(v, n % 128, 1)

    def edge_of(halo, p, s):
        return lane_roll(halo, -(32 * p + 7) if s > 0 else 103 - 32 * p)

    def shifted(main, halo, p, s):
        return jnp.where(lane == (0 if s > 0 else 127), edge_of(halo, p, s), lane_roll(main, s))

    def spread(f, q, t, halo, s):
        U[f, 16 + q, t] = halo
        UZ[f, 16 + q, t] = lane_roll(halo, s)
        XR[f, q, t] = lane_roll(halo, 32 * s)
        XZ[f, q, t] = lane_roll(halo, 33 * s)

    def neighbour(now, other, s):
        return jnp.where(segment == (0 if s > 0 else 3), other, now)

    def halves(group, planes, j):
        fields = [(n, e, w) for n, (e, w, s) in enumerate(fields_of(group)) if w % 7 != 6]
        members = list(enumerate(fields_of(group)))
        groups = {}
        for x in planes:
            groups.setdefault(x // 4, []).append(x)
        lone = range(10, 14)

        def put(ref, kept, f, unit, v):
            if j == 0 and unit in lone:
                ref[f, unit, 0], ref[f, unit, 1] = v, v
            elif j == 0:
                kept[f, unit] = v
                if unit in (8, 9, 14, 15):
                    ref[f, unit, 0], ref[f, unit, 1] = v, v
            else:
                own = kept[f, unit]
                ref[f, unit, 0], ref[f, unit, 1] = jnp.where(upper, own, v), jnp.where(upper, v, own)

        def main_of(x, e, w):
            if w % 7 == 3:
                return jnp.where(E[e + 3, x, j] > 0.5, E[e, x, j], FAR if w < 7 else -FAR)
            return E[e, x, j]

        for x in planes:
            for n, (e, w, _s) in members:
                TMP[n, x] = lane_roll(E[e, x, j], 8 + 16 * n)
                if w % 7 != 6:
                    put(U, N, PLACE[w], x, main_of(x, e, w))
                if group == SPUN:
                    s = SENSE[PLACE[w]]
                    edge = lane_roll(E[strip_of(group), x, j], -16 * n - 7 if s > 0 else 119 - 16 * n)
                    put(UZ, NZ, PLACE[w], x, jnp.where(lane == (0 if s > 0 else 127), edge, lane_roll(E[e, x, j], s)))
        for x in planes:
            strips = E[strip_of(group), x, j]
            edges = jnp.zeros((8, 128), jnp.float32)
            for n, _m in members:
                edges = jnp.where(quarter_low == n, TMP[n, x], edges)
            for side, v in enumerate((jnp.where(third, edges, strips), jnp.where(third, strips, edges))):
                if group == DISPLACED:
                    held = lane_roll(v, -48) > 0.5
                    v = jnp.where((quarter_low % 4 == 0) & ~held, jnp.where(lane < 64, FAR, -FAR), v)
                LR[side, x] = v
        for x in planes:
            low, high = LR[0, x], LR[1, x]
            for n, _e, _w in fields:
                at = 32 * (x % 4) - 16 * n
                TMP[n, x] = jnp.where(quarter_low % 2 == 0, lane_roll(low, at), lane_roll(high, at + 16))
        for q, places in groups.items():
            for n, e, w in fields:
                f = PLACE[w]
                v = TMP[n, places[0]]
                for x in places[1:]:
                    v = jnp.where(segment == x % 4, TMP[n, x], v)
                HALO[f, q] = v
                put(U, N, f, 16 + q, v)
        for q, places in groups.items():
            for n, e, w in fields:
                f = PLACE[w]
                s = SENSE[f]
                if s:
                    v = HALO[f, q]
                    put(UZ, NZ, f, 16 + q, lane_roll(v, s))
                    put(XR, NR, f, q, lane_roll(v, 32 * s))
                    put(XZ, NX, f, q, lane_roll(v, 33 * s))
                    if group == DISPLACED:
                        for x in places:
                            put(UZ, NZ, f, x, shifted(main_of(x, e, w), v, x % 4, s))

    def unpack_planes(group):
        for e in arrays_of(group):
            for i in range(2):
                v = RX[i, e]
                E[e, 10 + 2 * i, 0], E[e, 11 + 2 * i, 0] = v, swap(v)

    def unpack_corners(group):
        for e in arrays_of(group):
            for i in range(2):
                v = RC[i, e]
                E[e, 8 + 6 * i, 1], E[e, 9 + 6 * i, 1] = swap(v), v

    def before(x):
        return lax.rem(x + 15, 16)

    def after(x):
        return lax.rem(x + 1, 16)

    def group_at(q, n):
        return (q + n) % 4 if isinstance(q, int) else lax.rem(q + n, 4)

    def main_pair(f, x, oz):
        ref = UZ if oz else U
        return ref[f, x, 0], ref[f, x, 1]

    def halo_pair(f, q, ox, oz):
        if ox == 0:
            return main_pair(f, 16 + q, oz)
        ref = XZ if oz else XR
        s = SENSE[f]
        other = group_at(q, 3 if s > 0 else 1)
        return tuple(neighbour(ref[f, q, t], ref[f, other, t], s) for t in range(2))

    def bond_of(get, here, t, o):
        d = []
        for k in range(3):
            pair = get(D1 + k, o[0], o[2])
            v = below(pair, t) if o[1] else pair[t]
            d.append((v - here[k]) + (0.5 - o[k]))
        return d

    def bonds(get, unit, crossing=False):
        for t in range(2):
            here = [U[D0 + k, unit, t] for k in range(3)]
            for i, o in enumerate(corner_offsets):
                if crossing and not o[0]:
                    continue
                d = bond_of(get, here, t, o)
                r2 = d[0] * d[0] + d[1] * d[1] + d[2] * d[2]
                inverse = lax.rsqrt(r2)
                stretch = r2 * inverse - bond_length
                J[i, unit, t] = (0.25 * step_time * exchange_scale) * jnp.exp(-exchange_decay * stretch)
                P3[i, unit, t] = jnp.exp(-density_decay * stretch)
                RI[i, unit, t] = inverse

    def main_get(x):
        planes = (x, before(x))
        return lambda f, ox, oz: main_pair(f, planes[ox], oz)

    def halo_get(q):
        return lambda f, ox, oz: halo_pair(f, q, ox, oz)

    def main_bonds(x, _):
        bonds(main_get(x), x)
        return 0

    def halo_bonds(q, _):
        bonds(halo_get(q), 16 + q)
        return 0

    def halo_above(ref, i, q, ox, oz):
        if ox == 0:
            return [lane_roll(ref[i, 16 + q, t], -oz) if oz else ref[i, 16 + q, t] for t in range(2)]
        return [neighbour(lane_roll(ref[i, 16 + q, t], -32 - oz), lane_roll(ref[i, 16 + group_at(q, 1), t], -32 - oz), -1)
                for t in range(2)]

    def upper_bonds(q, _):
        following = group_at(q, 1)
        for i, o in enumerate(corner_offsets):
            pair = halo_above(J, i, q, o[0], o[2])
            for t in range(2):
                J1[i, 16 + q, t] = above(pair, t) if o[1] else pair[t]
            for p in [p for p in range(4) if 4 * q + p not in (11, 12)]:
                n = p + o[0]
                x = 4 * q + n if n < 4 else 4 * following
                halo = 16 + (q if n < 4 else following)
                pair = [J[i, x, t] for t in range(2)]
                if o[2]:
                    pair = [shifted(pair[t], J[i, halo, t], n % 4, -1) for t in range(2)]
                for t in range(2):
                    J1[i, 4 * q + p, t] = above(pair, t) if o[1] else pair[t]
        return 0

    def slope(rho):
        return -0.5 * lax.rsqrt(1.0 + rho)

    def own_slopes(units):
        for unit in units:
            for t in range(2):
                F0[unit, t] = slope(functools.reduce(jnp.add, [P3[i, unit, t] for i in range(8)]))

    def slopes(q, places):
        following = group_at(q, 1)
        high = []
        rows = []
        for oy in range(2):
            far = [halo_above(P3, 4 + 2 * oy + oz, q, 1, 0) for oz in range(2)]
            flat = [P3[2 * oy, 16 + q, t] + far[0][t] for t in range(2)]
            high.append([P3[2 * oy + 1, 16 + q, t] + far[1][t] for t in range(2)])
            rows.append([flat[t] + lane_roll(high[oy][t], -1) for t in range(2)])
        halo = [slope(rows[0][t] + above(rows[1], t)) for t in range(2)]
        for t in range(2):
            spread(FS, q, t, halo[t], 1)
        for p in places:
            x = 4 * q + p
            x1 = 4 * q + p + 1 if p < 3 else 4 * following
            rows = []
            for oy in range(2):
                total = []
                for t in range(2):
                    flat = P3[2 * oy, x, t] + P3[4 + 2 * oy, x1, t]
                    top = P3[2 * oy + 1, x, t] + P3[5 + 2 * oy, x1, t]
                    total.append(flat + shifted(top, high[oy][t], p, -1))
                rows.append(total)
            for t in range(2):
                v = slope(rows[0][t] + above(rows[1], t))
                U[FS, x, t] = v
                UZ[FS, x, t] = shifted(v, halo[t], p, 1)

    near, far, corner = tuple(range(8)), tuple(range(8, 16)), (8, 9, 14, 15)
    halves(DISPLACED, near, 0)
    halves(SPUN, near, 0)
    for c in xs0:
        c.wait()
    unpack_planes(DISPLACED)
    halves(DISPLACED, far, 0)
    for c in xs1:
        c.wait()
    unpack_planes(SPUN)
    halves(SPUN, far, 0)
    for c in ys0:
        c.wait()
    for e in arrays_of(DISPLACED):
        unpack_rows(e)
    corners0 = corner_copies(28, DISPLACED)
    halves(DISPLACED, near, 1)
    lax.fori_loop(0, 8, main_bonds, 0)
    lax.fori_loop(0, 2, halo_bonds, 0)
    lax.fori_loop(10, 12, main_bonds, 0)
    main_bonds(13, 0)
    upper_bonds(0, 0)
    slopes(0, range(4))
    own_slopes((1, 2, 3, 4, 5, 6, 7, 17))
    for c in ys1:
        c.wait()
    for e in arrays_of(SPUN):
        unpack_rows(e)
    corners1 = corner_copies(30, SPUN)
    halves(SPUN, near, 1)
    for c in corners0:
        c.wait()
    unpack_corners(DISPLACED)
    halves(DISPLACED, corner, 1)
    bonds(main_get(0), 0, True)
    lax.fori_loop(8, 10, main_bonds, 0)
    lax.fori_loop(14, 16, main_bonds, 0)
    lax.fori_loop(2, 5, lambda n, c: halo_bonds(group_at(n, 0), c), 0)
    for q in range(1, 4):
        upper_bonds(q, 0)
    for q, places in ((3, (3,)), (1, range(4)), (2, (0,))):
        slopes(q, places)
    own_slopes((0, 8, 16, 18))
    for c in corners1:
        c.wait()
    unpack_corners(SPUN)
    halves(SPUN, corner, 1)
    field_load.wait()
    outer = [(0.25 * step_time) * field[k] for k in range(3)]

    def cross(a, b):
        return [a[1] * b[2] - a[2] * b[1], a[2] * b[0] - a[0] * b[2], a[0] * b[1] - a[1] * b[0]]

    def update(u):
        sector = u if u < 8 else 14 - u
        sub, quarter = sector % 2, sector // 2
        tile = quarter // 2
        source, target, step = (S1, S0, -1) if sub == 0 else (S0, S1, 1)
        coupling = J if sub == 0 else J1
        planes = turned_planes()[u]
        shift = below if sub == 0 else above
        s_new = SENSE[target]

        @functools.cache
        def around(k, x):
            found = {}
            for oz in range(2):
                pair = main_pair(source + k, x % 16, oz)
                found[0, oz], found[1, oz] = pair[tile], shift(pair, tile)
            return found

        def turned(get, unit):
            c = [coupling[i, unit, tile] for i in range(8)]
            h = []
            for k in range(3):
                total = outer[k]
                for i, o in enumerate(corner_offsets):
                    total = total + c[i] * get(k, o)
                h.append(total + total if u == 7 else total)
            s = [U[target + k, unit, tile] for k in range(3)]
            once = cross(h, s)
            twice = cross(h, once)
            factor = 2.0 / (1.0 + (h[0] * h[0] + h[1] * h[1] + h[2] * h[2]))
            return [s[k] + factor * (once[k] + twice[k]) for k in range(3)]

        halos = {}
        for q in sorted({x % 16 // 4 for x in planes}):
            found = {}
            for k in range(3):
                for ox in range(2):
                    for oz in range(2):
                        pair = halo_pair(source + k, q, ox, oz)
                        found[k, ox, 0, oz], found[k, ox, 1, oz] = pair[tile], shift(pair, tile)
            halos[q] = turned(lambda k, o: found[k, o[0], o[1], o[2]], 16 + q)
            for k in range(3):
                spread(target + k, q, tile, halos[q][k], s_new)
        for x in planes:
            unit = x % 16
            v = turned(lambda k, o: around(k, x + step * o[0])[o[1], o[2]], unit)
            for k in range(3):
                U[target + k, unit, tile] = v[k]
                UZ[target + k, unit, tile] = shifted(v[k], halos[unit // 4][k], unit % 4, s_new)

    for u in range(15):
        update(u)

    def strength(get, unit, t, i, o, here, spins, mine):
        d = bond_of(get, here, t, o)

        def at(f):
            pair = get(f, o[0], o[2])
            return below(pair, t) if o[1] else pair[t]

        align = functools.reduce(jnp.add, [spins[k] * at(S1 + k) for k in range(3)])
        p = P3[i, unit, t]
        g = (-density_decay * p * (p * (pair_decay * pair_scale / density_decay) + (mine + at(FS)))
             + (exchange_decay / (0.25 * step_time)) * J[i, unit, t] * align) * RI[i, unit, t]
        return [g * d[k] for k in range(3)]

    def of_unit(unit, t):
        return [U[D0 + k, unit, t] for k in range(3)], [U[S0 + k, unit, t] for k in range(3)], F0[unit, t]

    def halo_forces(q, _):
        for t in range(2):
            own = of_unit(16 + q, t)
            for i, o in enumerate(corner_offsets):
                if o[2]:
                    v = strength(halo_get(q), 16 + q, t, i, o, *own)
                    for k in range(3):
                        HP[i // 2, k, q, t] = v[k]
        return 0

    for q in range(3):
        halo_forces(q, 0)

    def forces(x, q, p, sides=(0, 1)):
        planes = (x, before(x))
        sums = [[None] * 2 for _ in range(3)]
        parts = {}
        for t in range(2):
            own = of_unit(x, t)
            for i, o in enumerate(corner_offsets):
                if o[0] not in sides:
                    continue
                v = strength(main_get(x), x, t, i, o, *own)
                for k in range(3):
                    parts[i, t, k] = v[k]
                    sums[k][t] = v[k] if sums[k][t] is None else sums[k][t] + v[k]
        for k in range(3):
            for t in range(2):
                ACC[k, x, t] = sums[k][t]
            for ox in sides:
                rows = [[parts[4 * ox + 2 * oy, t, k] + shifted(parts[4 * ox + 2 * oy + 1, t, k], HP[2 * ox + oy, k, q, t], p, -1) for t in range(2)]
                        for oy in range(2)]
                for t in range(2):
                    v = rows[0][t] + above(rows[1], t)
                    if ox == 0:
                        ACC[3 + k, x, t] = -v
                    else:
                        ACC[3 + k, planes[1], t] = ACC[3 + k, planes[1], t] - v

    def four_forces(q, _):
        for p in range(4):
            forces(4 * q + p, q, p)
        return 0

    lax.fori_loop(0, 2, four_forces, 0)
    forces(8, 2, 0, (1,))

    def write(x, _):
        for f in range(6):
            for ref, at, out in ((U, (S1 if f > 2 else S0) + f % 3, out_s), (ACC, f, out_f)):
                out[f // 3, f % 3, x] = jnp.where(upper, ref[at, x, 0], ref[at, x, 1])
        return 0

    lax.fori_loop(0, 8, write, 0, unroll=4)


def emit(spins, forces, out_s, out_f, sem):
    copies = [pltpu.make_async_copy(a, b, sem.at[i]) for i, (a, b) in enumerate(((spins, out_s), (forces, out_f)))]
    for c in copies:
        c.start()
    for c in copies:
        c.wait()


def on_device(sizes, spin_vectors, displacement, occupied, applied_field):
    vmem = pl.BlockSpec(memory_space=pltpu.VMEM)
    hbm = pl.BlockSpec(memory_space=pltpu.HBM)
    shape = jax.ShapeDtypeStruct(spin_vectors.shape, jnp.float32)

    def buffer(*lead):
        return pltpu.VMEM(lead + (8, 128), jnp.float32)

    results = pl.pallas_call(
        functools.partial(kernel, sizes),
        out_shape=(pltpu.VMEM(shape.shape, jnp.float32),) * 2,
        in_specs=[hbm, hbm, hbm, hbm],
        out_specs=(vmem, vmem),
        scratch_shapes=[
            buffer(ARRAYS, 16, 2),
            buffer(2, 8), buffer(2, 2, 8),
            buffer(UP[-1]), buffer(UP[-1]),
            buffer(DOWN[-1]), buffer(DOWN[-1]),
            buffer(2, ARRAYS), buffer(2, ARRAYS),
            buffer(2, ARRAYS), buffer(2, ARRAYS),
            buffer(13, 20, 2), buffer(13, 20, 2), buffer(13, 4, 2), buffer(13, 4, 2), buffer(12, 20), buffer(12, 20), buffer(12, 4), buffer(12, 4), buffer(12, 4), buffer(2, 16), buffer(8, 16),
            buffer(8, 20, 2), buffer(8, 20, 2), buffer(8, 20, 2), buffer(8, 20, 2),
            buffer(20, 2), buffer(4, 3, 4, 2), buffer(6, 16, 2),
            pltpu.VMEM(spin_vectors.shape, jnp.float32),
            pltpu.VMEM(displacement.shape, jnp.float32),
            pltpu.VMEM(occupied.shape, jnp.int32),
            pltpu.SMEM(applied_field.shape, jnp.float32),
            pltpu.SemaphoreType.DMA((34,)),
            pltpu.SemaphoreType.DMA((34,)),
            pltpu.SemaphoreType.DMA((4,)),
        ],
        compiler_params=pltpu.CompilerParams(
            collective_id=0, has_side_effects=True, vmem_limit_bytes=60 * 1024 * 1024),
    )(spin_vectors, displacement, occupied, applied_field)
    return pl.pallas_call(
        emit,
        out_shape=(shape, shape),
        in_specs=[vmem, vmem],
        out_specs=(hbm, hbm),
        scratch_shapes=[pltpu.SemaphoreType.DMA((2,))],
        compiler_params=pltpu.CompilerParams(vmem_limit_bytes=4 * 1024 * 1024),
    )(*results)


def solution(mesh):
    sizes = tuple(mesh.shape[a] for a in axes)
    block = P(None, None, "gx", "gy", "gz")
    return jax.shard_map(
        functools.partial(on_device, sizes),
        mesh=mesh,
        in_specs=(block, block, P(None, "gx", "gy", "gz"), P()),
        out_specs=(block, block),
        check_vma=False,
    )
```
